32 devices in a mesh: groups: 2 (over y), tile: 8 (over z, x), feat: 2 (over core).
Axes of the slice: x: 2, y: 2, z: 4, core: 2. Of those that a mesh axis runs over, the one named last changes fastest.
Arguments:
- preacts: bfloat16 [3, 16384, 256], P(None, ('tile', 'feat'), 'groups'), parts along dimension 2, may hold values from -6 to 6
- targets: bfloat16 [3, 512, 1152], P(None, ('groups', 'tile', 'feat')), parts along dimension 1, may hold values from -4 to 4
- decoder: bfloat16 [16, 2, 12288, 2304], P(('groups', 'tile'), 'feat'), parts along dimension 0, may hold values from -0.02734375 to 0.02734375
- owner_list: int32 [16384, 6, 1], P(('tile', 'feat')), may hold values from 0 to 7; in each aligned block of 6144 rows (0 to 6143, 6144 to 12287, ..., all dimensions but the last counted through in order) at most 1536 rows name the same one
- tile_source: int32 [6], replicated, may hold values from 0 to 2, as said below
- tile_target: int32 [6], replicated, may hold values from 0 to 2, as said below
- row_order: int32 [4, 64], P('groups'), parts along dimension 0, may hold values from 0 to 63, each once within a row
Outputs:
- residual: float32 [3, 512, 1152], P(None, ('groups', 'tile', 'feat')), parts along dimension 1
- feature_grad: float32 [3, 16384, 256], P(None, ('tile', 'feat'), 'groups'), parts along dimension 2
The draws below stay inside these ranges and needn't reach their ends.
There are 2 independent parts, one for each index of `groups`. The reference program is written for one: setup_inputs(seed, part) draws one part's arguments, and reference() takes and returns one part's arrays. A program takes and returns all parts, laid end to end along the dimension named above; an argument that names none is the same for every part. Nothing has to cross between parts.
Inputs may be any that keep to these rules, and one draw needn't show every extreme that they name: `owner_list`: among the 6144 rows of one device (features f with f // 1024 equal, all tiles), no owner is named more than 1536 times, and in some device one owner exactly 1536 times; every owner is named somewhere. `tile_source`: together with tile_target, every pair of layers s <= t appears exactly once. tile_target[k] >= tile_source[k]. `row_order`: each row is a permutation.
All inputs are finite; a program needn't handle non-finite values.
Results may differ from the reference program's by a relative error of at most 0.0027.
Values may be sent and summed in bfloat16 or wider, within the bound.
No kernel may reach another device: no remote copies, remote signals or barrier semaphores. Data moves between devices by JAX's collectives and lax.ppermute only.
A program may use at most 128 MiB of HBM per device.

```python
import math
import jax
import jax.numpy as jnp
import numpy as np
from jax import lax

D = 2304
F = 16384
L = 3
NT = 6
NBLK = 2
TB = 64
TOK = 128
FPD = 1024
CAP = 1536
SLOTS = 12288
N_TILE = 8
N_FEAT = 2


def tile_pairs(key):
    pair_table = np.array([(source, target) for source in range(L) for target in range(source, L)], dtype=np.int32)
    shuffled = jax.random.permutation(jax.random.fold_in(key, 7), pair_table.shape[0])
    return jnp.asarray(pair_table)[shuffled]


def draw_tile_source(key, part):
    return tile_pairs(key)[:, 0].astype(jnp.int32)


def draw_tile_target(key, part):
    return tile_pairs(key)[:, 1].astype(jnp.int32)


def level_of(stream_key, dims, shards, low, high):
    def one(axis_at, blocks):
        steps = jax.random.uniform(jax.random.fold_in(jax.random.fold_in(stream_key, 6), axis_at), (blocks,), jnp.float32, low / len(shards), high / len(shards))
        return jnp.repeat(jnp.exp(steps), dims[axis_at] // blocks).reshape((-1,) + (1,) * (len(dims) - axis_at - 1))

    level = one(*shards[0])
    for cut in shards[1:]:
        level = level * one(*cut)
    return level


def deal_out(rng, own, number, rows, count, top, most, lean):
    order = jax.random.permutation(rng, count)
    heavy_load, usual = portions_of(count, rows * top, most, lean, True), portions_of(count, rows * top, most, lean, False)
    places = jnp.arange(count)

    def named(sizes, offset_by):
        used = int((sizes > 0).sum())
        fixed = max(1, used // 4)
        shifted = fixed + (places - fixed + offset_by * (used - fixed)) % max(1, count - fixed)
        return jnp.zeros((count,), jnp.int32).at[order[jnp.where(places < fixed, places, shifted)]].set(jnp.asarray(sizes, jnp.int32))

    sizes = jnp.where(number % 4 == 0, named(heavy_load, number // 4), named(usual, number - number // 4 - 1))
    mixed = jax.random.permutation(jax.random.fold_in(own, 3), count)
    giver, taker = mixed[0:count // 2 * 2:2], mixed[1:count // 2 * 2:2]
    margin = jnp.minimum(sizes[giver] - 1, most - sizes[taker]) // 2
    margin = jnp.where((giver == order[0]) | (taker == order[0]) | (sizes[taker] == 0), 0, jnp.maximum(margin, 0))
    shifted = jax.random.randint(jax.random.fold_in(own, 4), (count // 2,), 0, 1 << 20) % (margin + 1)
    sizes = sizes.at[giver].add(-shifted).at[taker].add(shifted)
    items = jnp.searchsorted(jnp.cumsum(sizes), jnp.arange(rows * top), side="right").astype(jnp.int32)
    listing = items.reshape(top, rows).T
    listing = listing[jax.random.permutation(jax.random.fold_in(own, 1), rows)]
    offset_by = jax.random.randint(jax.random.fold_in(own, 2), (rows, 1), 0, top)
    return jnp.take_along_axis(listing, (jnp.arange(top)[None, :] + offset_by) % top, axis=1)


def portions_of(count, total, most, lean, full):
    loads = [(1 << 20) // math.isqrt(standing ** lean) + 1 for standing in range(1, count + 1)]
    largest = most if full else min(most, max(-(-total // count), total * loads[0] // sum(loads)))
    least = 1 if total - largest >= count - 1 else 0
    holding, spare = [largest] + [least] * (count - 1), total - largest - least * (count - 1)
    while spare > 0:
        movable = [i for i in range(1, count) if holding[i] < largest] or [i for i in range(1, count) if holding[i] < most]
        mass, left = sum([loads[i] for i in movable]), spare
        for i in movable:
            extra = min(most - holding[i], max(1, left * loads[i] // mass), spare)
            holding[i] = holding[i] + extra
            spare = spare - extra
    return np.array(holding)


def bell_draw(stream_key, dims, scale, limit, cuts=(), kind=jnp.bfloat16):
    values = scale * jax.random.normal(stream_key, dims, jnp.float32)
    if cuts:
        values = values * level_of(stream_key, dims, cuts, -0.22, 0.18)
    return jnp.clip(values, -limit, limit).astype(kind)


def setup_inputs(seed: int = 0, part: int = 0) -> dict:
    key_of = jax.random.split(jax.random.key(seed), 8)
    part_splits = jax.random.split(jax.random.fold_in(key_of[7], part), 8)
    preacts = bell_draw(part_splits[0], (L, F, TOK), 1.0, 6.0, ((1, 16),))
    targets = bell_draw(part_splits[1], (L, 2 * TOK, D // 2), 0.5, 4.0, ((1, 16),))
    decoder = bell_draw(part_splits[2], (N_TILE, N_FEAT, SLOTS, D), (L * F) ** -0.5, 0.02734375, ((0, 8), (1, 2)))
    owner_list_keys = jax.random.split(jax.random.fold_in(key_of[3], 1), F * NT // (NT * FPD))
    owner_list_turns = jax.random.permutation(jax.random.fold_in(key_of[3], 3), F * NT // (NT * FPD))
    owner_list = jax.vmap(lambda own, number: deal_out(jax.random.fold_in(key_of[3], 2), own, number, NT * FPD, N_TILE, 1, CAP, 2))(owner_list_keys, owner_list_turns).reshape((F, NT, 1))
    tile_source = draw_tile_source(jax.random.fold_in(key_of[7], 71), part)
    tile_target = draw_tile_target(jax.random.fold_in(key_of[7], 71), part)
    row_order = jax.vmap(lambda own: jax.random.permutation(own, TB))(jax.random.split(part_splits[6], NBLK)).reshape((NBLK, TB)).astype(jnp.int32)
    return dict(preacts=preacts, targets=targets, decoder=decoder, owner_list=owner_list, tile_source=tile_source, tile_target=tile_target, row_order=row_order)


def reorder(values, indices):
    leading = values.shape[:-1]
    blocks, block_span = indices.shape
    shaped = values.reshape(leading + (blocks, block_span))
    block_col = jnp.arange(blocks, dtype=jnp.int32)[:, None]
    return shaped[..., block_col, indices].reshape(values.shape)


def inverse_order(row_order):
    positions = lax.broadcasted_iota(jnp.int32, row_order.shape, 1)
    block_ids = lax.broadcasted_iota(jnp.int32, row_order.shape, 0)
    inverse = jnp.zeros(row_order.shape, jnp.int32)
    return inverse.at[block_ids, row_order.astype(jnp.int32)].set(positions)


def reference(preacts, targets, decoder, owner_list, tile_source, tile_target, row_order):
    devices_all = N_TILE * N_FEAT
    feat_dev = F // devices_all
    tile_count = tile_source.shape[0]
    active = jax.nn.relu(preacts.astype(jnp.float32)).astype(jnp.bfloat16)
    natural = reorder(active, inverse_order(row_order))
    count_rows = feat_dev * tile_count
    destination = owner_list.reshape(devices_all, count_rows).astype(jnp.int32)
    same_owner = destination[:, :, None] == destination[:, None, :]
    before = lax.broadcasted_iota(jnp.int32, (count_rows, count_rows), 0) < lax.broadcasted_iota(jnp.int32, (count_rows, count_rows), 1)
    slot_rank = jnp.sum((same_owner & before[None]).astype(jnp.int32), axis=1)
    device_ids = lax.broadcasted_iota(jnp.int32, (devices_all, count_rows), 0)
    owner_src = device_ids // N_FEAT
    feat_half = device_ids % N_FEAT
    flat_index = ((destination * N_FEAT + feat_half) * SLOTS + owner_src * CAP + slot_rank).reshape(-1)
    weight_table = decoder.reshape(-1, D)
    row_weights = weight_table[flat_index].reshape(F, tile_count, D)
    layer_ids = jnp.arange(L, dtype=jnp.int32)[:, None, None]
    recon = jnp.zeros((L, TOK, D), jnp.float32)
    for tile_id in range(tile_count):
        product = lax.dot_general(natural[tile_source[tile_id]], row_weights[:, tile_id], (((0,), (0,)), ((), ())), preferred_element_type=jnp.float32)
        recon = recon + jnp.where(layer_ids == tile_target[tile_id], product[None], 0.0)
    residual = recon.reshape(L, 2 * TOK, D // 2) - targets.astype(jnp.float32)
    spread = residual.astype(jnp.bfloat16).reshape(L, TOK, D)
    layer_grad = jnp.zeros((L, F, TOK), jnp.float32)
    for tile_id in range(tile_count):
        product = lax.dot_general(row_weights[:, tile_id], spread[tile_target[tile_id]], (((1,), (1,)), ((), ())), preferred_element_type=jnp.float32)
        layer_grad = layer_grad + jnp.where(layer_ids == tile_source[tile_id], product[None], 0.0)
    natural_pre = reorder(preacts, inverse_order(row_order))
    layer_grad = jnp.where(natural_pre > 0, layer_grad, 0.0)
    return residual, reorder(layer_grad, row_order.astype(jnp.int32))
```

```python
import functools

import jax
import jax.numpy as jnp
from jax import lax
from jax.experimental import pallas as pl
from jax.experimental.pallas import tpu as pltpu
from jax.sharding import PartitionSpec as P


META = 16
UNROLL = 8
NCOL = 768
SPLIT = 2
SEND_ORDER = (4, 1, 2, 3, 5, 6, 7)
FORWARD_RUNS = ((0,), (1, 2, 3), (4, 5), (6,), (7,))
BACKWARD_RUNS = ((4,), (5,), (6, 7), (3, 2, 1, 0))


def reorder(values, indices):
    leading = values.shape[:-1]
    blocks, block_span = indices.shape
    shaped = values.reshape(leading + (blocks, block_span))
    block_col = jnp.arange(blocks, dtype=jnp.int32)[:, None]
    return shaped[..., block_col, indices].reshape(values.shape)


def inverse_order(row_order):
    positions = lax.broadcasted_iota(jnp.int32, row_order.shape, 1)
    block_ids = lax.broadcasted_iota(jnp.int32, row_order.shape, 0)
    inverse = jnp.zeros(row_order.shape, jnp.int32)
    return inverse.at[block_ids, row_order].set(positions)


def on_device_general(preacts, targets, decoder, owner_list, tile_source, tile_target, row_order):
    owners = lax.axis_size("tile")
    layers, feat_dev, tokens = preacts.shape
    tile_count = tile_source.shape[0]
    slot_count = decoder.shape[2]
    capacity = slot_count // owners
    model_width = decoder.shape[3]
    inverse = inverse_order(row_order)
    active = jax.nn.relu(preacts.astype(jnp.float32)).astype(jnp.bfloat16)
    natural = reorder(active, inverse)
    picked = natural[tile_source]
    row_values = jnp.transpose(picked, (1, 0, 2)).reshape(feat_dev * tile_count, tokens)
    destination = owner_list.reshape(-1)
    count_rows = destination.shape[0]
    same_owner = destination[:, None] == destination[None, :]
    before = lax.broadcasted_iota(jnp.int32, (count_rows, count_rows), 0) < lax.broadcasted_iota(
        jnp.int32, (count_rows, count_rows), 1
    )
    slot_rank = jnp.sum((same_owner & before).astype(jnp.int32), axis=0)
    slot_of = destination * capacity + slot_rank
    slot_match = lax.broadcasted_iota(jnp.int32, (slot_count, count_rows), 0) == slot_of[None, :]
    packed = jnp.dot(
        slot_match.astype(jnp.bfloat16), row_values, preferred_element_type=jnp.float32
    ).astype(jnp.bfloat16)
    tile_of_row = lax.broadcasted_iota(jnp.int32, (feat_dev, tile_count), 1).reshape(-1)
    tile_slot = jnp.sum(jnp.where(slot_match, tile_of_row[None, :] + 1, 0), axis=1) - 1
    received, tile_recv = (
        lax.all_to_all(
            packed.reshape(owners, capacity, tokens),
            "tile",
            split_axis=0,
            concat_axis=0,
            tiled=True,
        ),
        lax.all_to_all(
            tile_slot.reshape(owners, capacity), "tile", split_axis=0, concat_axis=0, tiled=True
        ),
    )
    received = received.reshape(slot_count, tokens)
    tile_recv = tile_recv.reshape(slot_count)
    tile_ids = lax.broadcasted_iota(jnp.int32, (slot_count, tile_count), 1)
    target_slot = jnp.sum(
        jnp.where(tile_recv[:, None] == tile_ids, tile_target[None, :], 0), axis=1
    )
    occupied = tile_recv >= 0
    weights = decoder[0, 0]
    pieces = []
    for target_layer in range(layers):
        chosen = (occupied & (target_slot == target_layer))[:, None]
        masked = jnp.where(chosen, received, jnp.zeros_like(received))
        pieces.append(
            lax.dot_general(
                masked, weights, (((0,), (0,)), ((), ())), preferred_element_type=jnp.float32
            )
        )
    partial_value = jnp.stack(pieces).reshape(layers, 2 * tokens, model_width // 2)
    own_sums = lax.psum_scatter(partial_value, ("tile", "feat"), scatter_dimension=1, tiled=True)
    residual = own_sums - targets.astype(jnp.float32)
    spread = lax.all_gather(
        residual.astype(jnp.bfloat16), ("tile", "feat"), axis=1, tiled=True
    ).reshape(layers, tokens, model_width)
    slot_grad = jnp.zeros((slot_count, tokens), jnp.float32)
    for target_layer in range(layers):
        chosen = (occupied & (target_slot == target_layer))[:, None]
        product = lax.dot_general(
            weights,
            spread[target_layer],
            (((1,), (1,)), ((), ())),
            preferred_element_type=jnp.float32,
        )
        slot_grad = slot_grad + jnp.where(chosen, product, 0.0)
    returned = lax.all_to_all(
        slot_grad.reshape(owners, capacity, tokens), "tile", split_axis=0, concat_axis=0, tiled=True
    ).reshape(slot_count, tokens)
    row_grad = returned[slot_of].reshape(feat_dev, tile_count, tokens)
    layer_grad = jnp.stack(
        [
            jnp.sum(jnp.where((tile_source == source_layer)[None, :, None], row_grad, 0.0), axis=1)
            for source_layer in range(layers)
        ]
    )
    natural_pre = reorder(preacts, inverse)
    layer_grad = jnp.where(natural_pre > 0, layer_grad, 0.0)
    feature_grad = reorder(layer_grad, row_order)
    return (residual, feature_grad)


def vmem(limit=60):
    return pltpu.CompilerParams(vmem_limit_bytes=limit * 2**20)


def full(shape):
    return pl.BlockSpec(shape, lambda *_: (0,) * len(shape))


def pack_kernel(slot_sm, src_sm, pre_ref, perm_ref, meta_ref, *refs):
    outs, (nat, packed) = refs[:-2], refs[-2:]
    layers, feats, _ = pre_ref.shape
    tiles = src_sm.shape[0]
    capacity = packed.shape[0] // len(outs)
    for s in range(layers):
        active = jnp.maximum(pre_ref[s].astype(jnp.float32), 0.0).astype(jnp.bfloat16)
        nat[pl.ds(s * feats, feats), :] = jnp.dot(
            active, perm_ref[...], preferred_element_type=jnp.float32
        )
    bases = [src_sm[k] * feats for k in range(tiles)]

    def step(i, carry):
        for j in range(UNROLL):
            f = i * UNROLL + j
            for k in range(tiles):
                slot = slot_sm[f * tiles + k]
                packed[pl.ds(slot, 1), :] = nat[pl.ds(bases[k] + f, 1), :]
        return carry

    lax.fori_loop(0, feats // UNROLL, step, 0)
    for d, out_ref in enumerate(outs):
        out_ref[:capacity, :] = packed[d * capacity : (d + 1) * capacity, :].astype(jnp.bfloat16)
        out_ref[capacity:, :] = meta_ref[d]


def slot_targets(meta, tgt_sm):
    values = meta.astype(jnp.float32)
    target = jnp.full(values.shape, -1.0, jnp.float32)
    for k in range(tgt_sm.shape[0]):
        target = jnp.where(values == float(k + 1), tgt_sm[k].astype(jnp.float32), target)
    return target


def forward_kernel(count, first, last, tgt_sm, seq_sm, me_sm, half_sm, *refs):
    recv_refs, w_ref, refs = refs[:count], refs[count], refs[count + 1 :]
    if not first:
        before_ref, refs = refs[0], refs[1:]
    outs, (acc, lhs, goal, stage) = refs[:-4], refs[-4:]
    i = pl.program_id(0)
    depth, width = w_ref.shape
    capacity = depth * SPLIT
    tokens = recv_refs[0].shape[1]
    layers = lhs.shape[0] // tokens
    groups = depth // 128
    for n in range(count * SPLIT):

        @pl.when(i == n)
        def _():
            recv_ref, first_row = recv_refs[n // SPLIT], n % SPLIT * groups
            target = slot_targets(recv_ref[capacity:, :], tgt_sm)
            goal[:groups, :] = target[first_row : first_row + groups, :]
            stage[...] = recv_ref[first_row * 128 : (first_row + groups) * 128, :]

    for j in range(groups):
        span = slice(j * 128, (j + 1) * 128)
        acts = stage[span, :].astype(jnp.float32).T
        for t in range(layers):
            lhs[t * tokens : (t + 1) * tokens, span] = jnp.where(
                goal[j : j + 1, :] == float(t), acts, 0.0
            ).astype(jnp.bfloat16)

    @pl.when(i == 0)
    def _():
        acc[...] = jnp.zeros_like(acc) if first else before_ref[...]

    for n in range(width // NCOL):
        cols = slice(n * NCOL, (n + 1) * NCOL)
        acc[:, cols] += jnp.dot(lhs[...], w_ref[:, cols], preferred_element_type=jnp.float32)

    @pl.when(i == count * SPLIT - 1)
    def _():
        if not last:
            outs[0][...] = acc[...]
            return
        owners = outs[0].shape[0]
        for d in range(owners):
            for t in range(layers):
                for side, half in enumerate((half_sm[0], 1 - half_sm[0])):
                    place = pl.multiple_of(t * tokens + (me_sm[0] ^ d) * 16 + half * 8, 8)
                    values = acc[pl.ds(place, 8), :]
                    if t < layers - 1:
                        outs[2 * side][d, t * 8 : (t + 1) * 8, :] = values
                    else:
                        outs[2 * side + 1][d] = values


def backward_kernel(count, first, tgt_sm, seq_sm, me_sm, *all_refs):
    refs = all_refs
    meta_refs, w_ref, refs = refs[:count], refs[count], refs[count + 1 : -2]
    goal, stage = all_refs[-2:]
    i = pl.program_id(0)
    if first:
        mine_ref, other_ref, place_ref = refs[:3]
        outs, spread = refs[3:-1], refs[-1]
        half = mine_ref.shape[0]

        @pl.when(i == 0)
        def _():
            spread[...] = (
                jnp.dot(place_ref[:, :half], mine_ref[...], preferred_element_type=jnp.float32)
                + jnp.dot(place_ref[:, half:], other_ref[...], preferred_element_type=jnp.float32)
            ).astype(jnp.bfloat16)

    else:
        spread, outs = refs[0], refs[1:]
    depth = w_ref.shape[0]
    tokens = outs[0].shape[1]
    layers = spread.shape[0] // tokens
    groups = depth // 128
    for n in range(count * SPLIT):

        @pl.when(i == n)
        def _():
            first_row = n % SPLIT * groups
            target = slot_targets(meta_refs[n // SPLIT][...], tgt_sm)
            goal[:groups, :] = target[first_row : first_row + groups, :]

    for j in range(depth // 256):
        grads = lax.dot_general(
            spread[...],
            w_ref[j * 256 : (j + 1) * 256, :],
            (((1,), (1,)), ((), ())),
            preferred_element_type=jnp.float32,
        )
        for h in range(2):
            row = goal[2 * j + h : 2 * j + h + 1, :]
            chosen = jnp.zeros((tokens, 128), jnp.float32)
            for t in range(layers):
                part = grads[t * tokens : (t + 1) * tokens, h * 128 : (h + 1) * 128]
                chosen = jnp.where(row == float(t), part, chosen)
            begin = j * 256 + h * 128
            stage[begin : begin + 128, :] = chosen.T.astype(jnp.bfloat16)
    for n in range(count * SPLIT):

        @pl.when(i == n)
        def _():
            outs[n // SPLIT][n % SPLIT * depth : (n % SPLIT + 1) * depth, :] = stage[...]


def unpack_kernel(slot_sm, order_sm, *refs):
    backs, (pre_ref, out_ref, rows) = refs[:-3], refs[-3:]
    layers, feats, _ = pre_ref.shape
    tiles = order_sm.shape[0]
    capacity = rows.shape[0] // len(backs)
    for d, back_ref in enumerate(backs):
        rows[d * capacity : (d + 1) * capacity, :] = back_ref[...].astype(jnp.float32)
    order = [order_sm[k] for k in range(tiles)]

    def step(i, carry):
        for j in range(UNROLL):
            f = i * UNROLL + j
            k = 0
            for s in range(layers):
                total = None
                for _ in range(layers - s):
                    row = rows[pl.ds(slot_sm[f * tiles + order[k]], 1), :]
                    total = row if total is None else total + row
                    k += 1
                out_ref[s, pl.ds(f, 1), :] = total
        return carry

    lax.fori_loop(0, feats // UNROLL, step, 0)
    for s in range(layers):
        out_ref[s] = jnp.where(pre_ref[s].astype(jnp.float32) > 0, out_ref[s], 0.0)


def slot_plan(owner_list, tile_count, owners, capacity):
    count = owner_list.size
    blocks = count // 128
    dest = owner_list.reshape(blocks, 128)
    same = dest[None] == lax.broadcasted_iota(jnp.int32, (owners, 1, 1), 0)
    ones = same.astype(jnp.bfloat16)
    lane = lax.broadcasted_iota(jnp.int32, (128, 128), 0) < lax.broadcasted_iota(
        jnp.int32, (128, 128), 1
    )
    ahead = lax.broadcasted_iota(jnp.int32, (blocks, blocks), 0) < lax.broadcasted_iota(
        jnp.int32, (blocks, blocks), 1
    )
    within = jnp.einsum(
        "pbi,ij->pbj", ones, lane.astype(jnp.bfloat16), preferred_element_type=jnp.float32
    )
    totals = jnp.sum(ones, axis=2, dtype=jnp.float32).astype(jnp.bfloat16)
    base = jnp.dot(totals, ahead.astype(jnp.bfloat16), preferred_element_type=jnp.float32)
    rank = jnp.sum(jnp.where(same, within + base[:, :, None], 0.0), axis=0).astype(jnp.int32)
    slot = (dest * capacity + rank).reshape(1, count)
    slots = owners * capacity
    tile = lax.broadcasted_iota(jnp.int32, (1, count), 1) % tile_count
    high = lax.broadcasted_iota(jnp.int32, (slots // 128, 1), 0) == slot // 128
    low = lax.broadcasted_iota(jnp.int32, (128, 1), 0) == slot % 128
    meta = lax.dot_general(
        jnp.where(high, (tile + 1).astype(jnp.bfloat16), 0),
        low.astype(jnp.bfloat16),
        (((1,), (1,)), ((), ())),
        preferred_element_type=jnp.float32,
    )
    meta = meta.reshape(owners, capacity // 128, 128).astype(jnp.bfloat16)
    meta = jnp.pad(meta, ((0, 0), (0, META - capacity // 128), (0, 0)))
    return slot.reshape(count), meta


def on_device_fast(*args):
    return fast_step(*args)


def fast_step(preacts, targets, decoder, owner_list, tile_source, tile_target, row_order):
    owners = lax.axis_size("tile")
    my_half = lax.axis_index("feat")
    layers, feats, tokens = preacts.shape
    tiles = tile_source.shape[0]
    slots, width = decoder.shape[2:]
    capacity = slots // owners
    rows = layers * 8
    weights = decoder.reshape(slots, width)
    bf16, f32, i32 = jnp.bfloat16, jnp.float32, jnp.int32

    me = lax.axis_index("tile")
    slot, meta = slot_plan(owner_list ^ me, tiles, owners, capacity)
    me_id = jnp.reshape(me, (1,)).astype(i32)
    half_id = jnp.reshape(my_half, (1,)).astype(i32)
    block_of = lax.broadcasted_iota(i32, row_order.shape, 0) * row_order.shape[1]
    token_of = (row_order + block_of).reshape(tokens)
    perm = (token_of[:, None] == lax.broadcasted_iota(i32, (1, tokens), 1)).astype(bf16)
    index = lax.broadcasted_iota(i32, (1, layers * tokens), 1)
    side = jnp.where(index // (owners * rows) == 0, my_half, 1 - my_half)
    held = (index % (owners * rows)) // rows * 16 + side * 8 + index % 8
    held_layer = index % rows // 8
    wanted = jnp.tile(token_of, layers)[:, None]
    wanted_layer = lax.broadcasted_iota(i32, (layers * tokens, 1), 0) // tokens
    place = ((held == wanted) & (held_layer == wanted_layer)).astype(bf16)
    tile_ids = jnp.arange(tiles, dtype=i32)
    earlier = (tile_source[None, :] < tile_source[:, None]) | (
        (tile_source[None, :] == tile_source[:, None]) & (tile_ids[None, :] < tile_ids[:, None])
    )
    position = jnp.sum(earlier.astype(i32), axis=1)
    order = jnp.sum(
        jnp.where(position[None, :] == tile_ids[:, None], tile_ids[None, :], 0), axis=1
    ).astype(i32)

    def to_peer(d, block):
        return lax.ppermute(block, "tile", [(q, q ^ d) for q in range(owners)])

    mirror = owners // 2
    near = range(1, mirror)
    block = jax.ShapeDtypeStruct((capacity + META, tokens), bf16)
    packed = pl.pallas_call(
        pack_kernel,
        out_shape=[block] * owners,
        grid_spec=pltpu.PrefetchScalarGridSpec(
            num_scalar_prefetch=2,
            grid=(1,),
            in_specs=[full(preacts.shape), full(perm.shape), full(meta.shape)],
            out_specs=[full(block.shape)] * owners,
            scratch_shapes=[
                pltpu.VMEM((layers * feats, tokens), f32),
                pltpu.VMEM((slots, tokens), f32),
            ],
        ),
        compiler_params=vmem(32),
    )(slot, tile_source, preacts, perm, meta)
    received = list(packed)
    for d in SEND_ORDER:
        received[d] = to_peer(d, packed[d])

    def cost(count):
        return pl.CostEstimate(
            flops=2 * layers * tokens * count * capacity * width,
            bytes_accessed=2 * count * capacity * width,
            transcendentals=0,
        )

    weight_spec = pl.BlockSpec(
        (capacity // SPLIT, width),
        lambda i, tgt, seq, me, *_: ((me[0] ^ seq[i // SPLIT]) * SPLIT + i % SPLIT, 0),
    )
    whole = pl.BlockSpec(memory_space=pltpu.VMEM)

    def forward(run, before, last):
        first, count = before is None, len(run)
        if last:
            outs = [
                jax.ShapeDtypeStruct((owners, rows - 8, width), f32),
                jax.ShapeDtypeStruct((owners, 8, width), f32),
            ] * 2
        else:
            outs = [jax.ShapeDtypeStruct((layers * tokens, width), f32)]
        sums = [] if first else [before]
        return pl.pallas_call(
            functools.partial(forward_kernel, count, first, last),
            out_shape=outs,
            grid_spec=pltpu.PrefetchScalarGridSpec(
                num_scalar_prefetch=4,
                grid=(count * SPLIT,),
                in_specs=[whole] * count + [weight_spec] + [whole] * len(sums),
                out_specs=[whole] * len(outs),
                scratch_shapes=[
                    pltpu.VMEM((layers * tokens, width), f32),
                    pltpu.VMEM((layers * tokens, capacity // SPLIT), bf16),
                    pltpu.VMEM((META, 128), f32),
                    pltpu.VMEM((capacity // SPLIT, tokens), bf16),
                ],
            ),
            compiler_params=vmem(28),
            cost_estimate=cost(count),
        )(
            tile_target,
            jnp.array(run, i32),
            me_id,
            half_id,
            *[received[d] for d in run],
            weights,
            *sums,
        )

    value = None
    for number, run in enumerate(FORWARD_RUNS):
        last = number == len(FORWARD_RUNS) - 1
        value = forward(run, value, last)
        if not last:
            value = value[0]

    swap = [(0, 1), (1, 0)]
    keep_most, keep_last, send_most, send_last = value
    got_last = lax.ppermute(send_last, "feat", swap)
    got_most = lax.ppermute(send_most, "feat", swap)
    last_sum = keep_last + got_last
    across = to_peer(mirror, last_sum[mirror:])
    most_sum = (keep_most + got_most).reshape(2, mirror, rows - 8, width)
    pair = most_sum[:, 0]
    for d in near:
        pair = pair + to_peer(d, most_sum[:, d])
    last_sum = last_sum[:mirror] + across
    own_last = last_sum[0]
    for d in near:
        own_last = own_last + to_peer(d, last_sum[d])
    own_most = pair[0] + to_peer(mirror, pair[1])
    residual = jnp.concatenate([own_most, own_last]) - targets.astype(f32).reshape(rows, width)
    mine = lax.all_to_all(
        jnp.broadcast_to(residual.astype(bf16)[None], (owners, rows, width)),
        "tile",
        split_axis=0,
        concat_axis=0,
        tiled=True,
    ).reshape(owners * rows, width)
    other = lax.ppermute(mine, "feat", swap)

    grad_block = jax.ShapeDtypeStruct((capacity, tokens), bf16)
    spread_type = jax.ShapeDtypeStruct((layers * tokens, width), bf16)
    meta_spec = pl.BlockSpec((META, tokens), lambda *_: (capacity // META, 0))

    def backward(run, known):
        first, count = len(known) > 1, len(run)
        outs = [grad_block] * count + ([spread_type] if first else [])
        return pl.pallas_call(
            functools.partial(backward_kernel, count, first),
            out_shape=outs,
            grid_spec=pltpu.PrefetchScalarGridSpec(
                num_scalar_prefetch=3,
                grid=(count * SPLIT,),
                in_specs=[meta_spec] * count + [weight_spec] + [whole] * len(known),
                out_specs=[whole] * len(outs),
                scratch_shapes=[
                    pltpu.VMEM((META, 128), f32),
                    pltpu.VMEM((capacity // SPLIT, tokens), bf16),
                ],
            ),
            compiler_params=vmem(28),
            cost_estimate=cost(count),
        )(
            tile_target,
            jnp.array(run, i32),
            me_id,
            *[received[d] for d in run],
            weights,
            *known,
        )

    returned = [None] * owners
    known = (mine, other, place)
    for run in BACKWARD_RUNS:
        grads = backward(run, known)
        if len(known) > 1:
            known = (grads[len(run)],)
        for d, grad in zip(run, grads):
            returned[d] = to_peer(d, grad) if d else grad

    feature_grad = pl.pallas_call(
        unpack_kernel,
        out_shape=jax.ShapeDtypeStruct(preacts.shape, f32),
        grid_spec=pltpu.PrefetchScalarGridSpec(
            num_scalar_prefetch=2,
            grid=(1,),
            in_specs=[full(grad_block.shape)] * owners + [full(preacts.shape)],
            out_specs=full(preacts.shape),
            scratch_shapes=[pltpu.VMEM((slots, tokens), f32)],
        ),
        compiler_params=vmem(32),
    )(slot, order, *returned, preacts)
    return residual.reshape(targets.shape), feature_grad


def on_device(preacts, targets, decoder, owner_list, tile_source, tile_target, row_order):
    args = (preacts, targets, decoder, owner_list, tile_source, tile_target, row_order)
    owners, halves = lax.axis_size("tile"), lax.axis_size("feat")
    layers, feat_dev, tokens = preacts.shape
    tile_count = tile_source.shape[0]
    slot_count, model_width = decoder.shape[2:]
    fits = (
        tokens == 128
        and halves == 2
        and tokens == 8 * owners * halves
        and slot_count % (owners * 256) == 0
        and slot_count <= owners * META * 128
        and (feat_dev * tile_count) % 128 == 0
        and feat_dev % UNROLL == 0
        and tile_count * 2 == layers * (layers + 1)
        and model_width % 256 == 0
    )
    return (on_device_fast if fits else on_device_general)(*args)


def solution(mesh):
    return jax.shard_map(
        on_device,
        mesh=mesh,
        in_specs=(
            P(None, ("tile", "feat"), "groups"),
            P(None, ("groups", "tile", "feat"), None),
            P(("groups", "tile"), "feat", None, None),
            P(("tile", "feat"), None, None),
            P(),
            P(),
            P("groups", None),
        ),
        out_specs=(P(None, ("groups", "tile", "feat"), None), P(None, ("tile", "feat"), "groups")),
        check_vma=False,
    )
```

```python
import functools

import jax
import jax.numpy as jnp
from jax import lax
from jax.experimental import pallas as pl
from jax.experimental.pallas import tpu as pltpu
from jax.sharding import PartitionSpec as P


META = 16
UNROLL = 8
NCOL = 768
SPLIT = 2
SEND_ORDER = (2, 1, 3, 4, 5, 6, 7)
FORWARD_RUNS = ((0,), (1, 2, 3), (4, 5), (6,), (7,))
BACKWARD_RUNS = ((4,), (5,), (6, 7), (3, 2, 1, 0))


def reorder(values, indices):
    leading = values.shape[:-1]
    blocks, block_span = indices.shape
    shaped = values.reshape(leading + (blocks, block_span))
    block_col = jnp.arange(blocks, dtype=jnp.int32)[:, None]
    return shaped[..., block_col, indices].reshape(values.shape)


def inverse_order(row_order):
    positions = lax.broadcasted_iota(jnp.int32, row_order.shape, 1)
    block_ids = lax.broadcasted_iota(jnp.int32, row_order.shape, 0)
    inverse = jnp.zeros(row_order.shape, jnp.int32)
    return inverse.at[block_ids, row_order].set(positions)


def on_device_general(preacts, targets, decoder, owner_list, tile_source, tile_target, row_order):
    owners = lax.axis_size("tile")
    layers, feat_dev, tokens = preacts.shape
    tile_count = tile_source.shape[0]
    slot_count = decoder.shape[2]
    capacity = slot_count // owners
    model_width = decoder.shape[3]
    inverse = inverse_order(row_order)
    active = jax.nn.relu(preacts.astype(jnp.float32)).astype(jnp.bfloat16)
    natural = reorder(active, inverse)
    picked = natural[tile_source]
    row_values = jnp.transpose(picked, (1, 0, 2)).reshape(feat_dev * tile_count, tokens)
    destination = owner_list.reshape(-1)
    count_rows = destination.shape[0]
    same_owner = destination[:, None] == destination[None, :]
    before = lax.broadcasted_iota(jnp.int32, (count_rows, count_rows), 0) < lax.broadcasted_iota(
        jnp.int32, (count_rows, count_rows), 1
    )
    slot_rank = jnp.sum((same_owner & before).astype(jnp.int32), axis=0)
    slot_of = destination * capacity + slot_rank
    slot_match = lax.broadcasted_iota(jnp.int32, (slot_count, count_rows), 0) == slot_of[None, :]
    packed = jnp.dot(
        slot_match.astype(jnp.bfloat16), row_values, preferred_element_type=jnp.float32
    ).astype(jnp.bfloat16)
    tile_of_row = lax.broadcasted_iota(jnp.int32, (feat_dev, tile_count), 1).reshape(-1)
    tile_slot = jnp.sum(jnp.where(slot_match, tile_of_row[None, :] + 1, 0), axis=1) - 1
    received, tile_recv = (
        lax.all_to_all(
            packed.reshape(owners, capacity, tokens),
            "tile",
            split_axis=0,
            concat_axis=0,
            tiled=True,
        ),
        lax.all_to_all(
            tile_slot.reshape(owners, capacity), "tile", split_axis=0, concat_axis=0, tiled=True
        ),
    )
    received = received.reshape(slot_count, tokens)
    tile_recv = tile_recv.reshape(slot_count)
    tile_ids = lax.broadcasted_iota(jnp.int32, (slot_count, tile_count), 1)
    target_slot = jnp.sum(
        jnp.where(tile_recv[:, None] == tile_ids, tile_target[None, :], 0), axis=1
    )
    occupied = tile_recv >= 0
    weights = decoder[0, 0]
    pieces = []
    for target_layer in range(layers):
        chosen = (occupied & (target_slot == target_layer))[:, None]
        masked = jnp.where(chosen, received, jnp.zeros_like(received))
        pieces.append(
            lax.dot_general(
                masked, weights, (((0,), (0,)), ((), ())), preferred_element_type=jnp.float32
            )
        )
    partial_value = jnp.stack(pieces).reshape(layers, 2 * tokens, model_width // 2)
    own_sums = lax.psum_scatter(partial_value, ("tile", "feat"), scatter_dimension=1, tiled=True)
    residual = own_sums - targets.astype(jnp.float32)
    spread = lax.all_gather(
        residual.astype(jnp.bfloat16), ("tile", "feat"), axis=1, tiled=True
    ).reshape(layers, tokens, model_width)
    slot_grad = jnp.zeros((slot_count, tokens), jnp.float32)
    for target_layer in range(layers):
        chosen = (occupied & (target_slot == target_layer))[:, None]
        product = lax.dot_general(
            weights,
            spread[target_layer],
            (((1,), (1,)), ((), ())),
            preferred_element_type=jnp.float32,
        )
        slot_grad = slot_grad + jnp.where(chosen, product, 0.0)
    returned = lax.all_to_all(
        slot_grad.reshape(owners, capacity, tokens), "tile", split_axis=0, concat_axis=0, tiled=True
    ).reshape(slot_count, tokens)
    row_grad = returned[slot_of].reshape(feat_dev, tile_count, tokens)
    layer_grad = jnp.stack(
        [
            jnp.sum(jnp.where((tile_source == source_layer)[None, :, None], row_grad, 0.0), axis=1)
            for source_layer in range(layers)
        ]
    )
    natural_pre = reorder(preacts, inverse)
    layer_grad = jnp.where(natural_pre > 0, layer_grad, 0.0)
    feature_grad = reorder(layer_grad, row_order)
    return (residual, feature_grad)


def vmem(limit=60):
    return pltpu.CompilerParams(vmem_limit_bytes=limit * 2**20)


def full(shape):
    return pl.BlockSpec(shape, lambda *_: (0,) * len(shape))


def pack_kernel(slot_sm, src_sm, pre_ref, perm_ref, meta_ref, *refs):
    outs, (nat, packed) = refs[:-2], refs[-2:]
    layers, feats, _ = pre_ref.shape
    tiles = src_sm.shape[0]
    capacity = packed.shape[0] // len(outs)
    for s in range(layers):
        active = jnp.maximum(pre_ref[s].astype(jnp.float32), 0.0).astype(jnp.bfloat16)
        nat[pl.ds(s * feats, feats), :] = jnp.dot(
            active, perm_ref[...], preferred_element_type=jnp.float32
        )
    bases = [src_sm[k] * feats for k in range(tiles)]

    def step(i, carry):
        for j in range(UNROLL):
            f = i * UNROLL + j
            for k in range(tiles):
                slot = slot_sm[f * tiles + k]
                packed[pl.ds(slot, 1), :] = nat[pl.ds(bases[k] + f, 1), :]
        return carry

    lax.fori_loop(0, feats // UNROLL, step, 0)
    for d, out_ref in enumerate(outs):
        out_ref[:capacity, :] = packed[d * capacity : (d + 1) * capacity, :].astype(jnp.bfloat16)
        out_ref[capacity:, :] = meta_ref[d]


def slot_targets(meta, tgt_sm):
    values = meta.astype(jnp.float32)
    target = jnp.full(values.shape, -1.0, jnp.float32)
    for k in range(tgt_sm.shape[0]):
        target = jnp.where(values == float(k + 1), tgt_sm[k].astype(jnp.float32), target)
    return target


def forward_kernel(count, first, last, ready, tgt_sm, seq_sm, me_sm, half_sm, *refs):
    recv_refs, w_ref, refs = refs[:count], refs[count], refs[count + 1 :]
    if not first:
        before_ref, refs = refs[0], refs[1 + ready :]
    outs, (acc, lhs, goal, stage) = refs[:-4], refs[-4:]
    i = pl.program_id(0)
    depth, width = w_ref.shape
    capacity = depth * SPLIT
    tokens = recv_refs[0].shape[1]
    layers = lhs.shape[0] // tokens
    groups = depth // 128
    for n in range(count * SPLIT):

        @pl.when(i == n)
        def _():
            recv_ref, first_row = recv_refs[n // SPLIT], n % SPLIT * groups
            target = slot_targets(recv_ref[capacity:, :], tgt_sm)
            goal[:groups, :] = target[first_row : first_row + groups, :]
            stage[...] = recv_ref[first_row * 128 : (first_row + groups) * 128, :]

    for j in range(groups):
        span = slice(j * 128, (j + 1) * 128)
        acts = stage[span, :].astype(jnp.float32).T
        for t in range(layers):
            lhs[t * tokens : (t + 1) * tokens, span] = jnp.where(
                goal[j : j + 1, :] == float(t), acts, 0.0
            ).astype(jnp.bfloat16)

    @pl.when(i == 0)
    def _():
        acc[...] = jnp.zeros_like(acc) if first else before_ref[...]

    for n in range(width // NCOL):
        cols = slice(n * NCOL, (n + 1) * NCOL)
        acc[:, cols] += jnp.dot(lhs[...], w_ref[:, cols], preferred_element_type=jnp.float32)

    @pl.when(i == count * SPLIT - 1)
    def _():
        if not last:
            outs[0][...] = acc[...]
            return
        owners = outs[0].shape[0]
        for d in range(owners):
            for t in range(layers):
                for side, half in enumerate((half_sm[0], 1 - half_sm[0])):
                    place = pl.multiple_of(t * tokens + (me_sm[0] ^ d) * 16 + half * 8, 8)
                    values = acc[pl.ds(place, 8), :]
                    if t < layers - 1:
                        outs[2 * side][d, t * 8 : (t + 1) * 8, :] = values
                    else:
                        outs[2 * side + 1][d] = values


def backward_kernel(count, first, tgt_sm, seq_sm, me_sm, *all_refs):
    refs = all_refs
    meta_refs, w_ref, refs = refs[:count], refs[count], refs[count + 1 : -2]
    goal, stage = all_refs[-2:]
    i = pl.program_id(0)
    if first:
        mine_ref, other_ref, place_ref = refs[:3]
        outs, spread = refs[3:-1], refs[-1]
        half = mine_ref.shape[0]

        @pl.when(i == 0)
        def _():
            spread[...] = (
                jnp.dot(place_ref[:, :half], mine_ref[...], preferred_element_type=jnp.float32)
                + jnp.dot(place_ref[:, half:], other_ref[...], preferred_element_type=jnp.float32)
            ).astype(jnp.bfloat16)

    else:
        spread, outs = refs[0], refs[1:]
    depth = w_ref.shape[0]
    tokens = outs[0].shape[1]
    layers = spread.shape[0] // tokens
    groups = depth // 128
    for n in range(count * SPLIT):

        @pl.when(i == n)
        def _():
            first_row = n % SPLIT * groups
            target = slot_targets(meta_refs[n // SPLIT][...], tgt_sm)
            goal[:groups, :] = target[first_row : first_row + groups, :]

    for j in range(depth // 256):
        grads = lax.dot_general(
            spread[...],
            w_ref[j * 256 : (j + 1) * 256, :],
            (((1,), (1,)), ((), ())),
            preferred_element_type=jnp.float32,
        )
        for h in range(2):
            row = goal[2 * j + h : 2 * j + h + 1, :]
            chosen = jnp.zeros((tokens, 128), jnp.float32)
            for t in range(layers):
                part = grads[t * tokens : (t + 1) * tokens, h * 128 : (h + 1) * 128]
                chosen = jnp.where(row == float(t), part, chosen)
            begin = j * 256 + h * 128
            stage[begin : begin + 128, :] = chosen.T.astype(jnp.bfloat16)
    for n in range(count * SPLIT):

        @pl.when(i == n)
        def _():
            outs[n // SPLIT][n % SPLIT * depth : (n % SPLIT + 1) * depth, :] = stage[...]


def unpack_kernel(slot_sm, order_sm, *refs):
    backs, (pre_ref, out_ref, rows, landed, sems) = refs[:-5], refs[-5:]
    layers, feats, _ = pre_ref.shape
    tiles = order_sm.shape[0]
    capacity = rows.shape[0] // len(backs)
    copies = [
        pltpu.make_async_copy(back_ref, landed.at[d], sems.at[d])
        for d, back_ref in enumerate(backs)
    ]
    for copy in copies:
        copy.start()
    for d, copy in enumerate(copies):
        copy.wait()
        rows[d * capacity : (d + 1) * capacity, :] = landed[d].astype(jnp.float32)
    order = [order_sm[k] for k in range(tiles)]

    def step(i, carry):
        for j in range(UNROLL):
            f = i * UNROLL + j
            k = 0
            for s in range(layers):
                total = None
                for _ in range(layers - s):
                    row = rows[pl.ds(slot_sm[f * tiles + order[k]], 1), :]
                    total = row if total is None else total + row
                    k += 1
                out_ref[s, pl.ds(f, 1), :] = total
        return carry

    lax.fori_loop(0, feats // UNROLL, step, 0)
    for s in range(layers):
        out_ref[s] = jnp.where(pre_ref[s].astype(jnp.float32) > 0, out_ref[s], 0.0)


def slot_plan(owner_list, tile_count, owners, capacity):
    count = owner_list.size
    blocks = count // 128
    dest = owner_list.reshape(blocks, 128)
    same = dest[None] == lax.broadcasted_iota(jnp.int32, (owners, 1, 1), 0)
    ones = same.astype(jnp.bfloat16)
    lane = lax.broadcasted_iota(jnp.int32, (128, 128), 0) < lax.broadcasted_iota(
        jnp.int32, (128, 128), 1
    )
    ahead = lax.broadcasted_iota(jnp.int32, (blocks, blocks), 0) < lax.broadcasted_iota(
        jnp.int32, (blocks, blocks), 1
    )
    within = jnp.einsum(
        "pbi,ij->pbj", ones, lane.astype(jnp.bfloat16), preferred_element_type=jnp.float32
    )
    totals = jnp.sum(ones, axis=2, dtype=jnp.float32).astype(jnp.bfloat16)
    base = jnp.dot(totals, ahead.astype(jnp.bfloat16), preferred_element_type=jnp.float32)
    rank = jnp.sum(jnp.where(same, within + base[:, :, None], 0.0), axis=0).astype(jnp.int32)
    slot = (dest * capacity + rank).reshape(1, count)
    slots = owners * capacity
    tile = lax.broadcasted_iota(jnp.int32, (1, count), 1) % tile_count
    high = lax.broadcasted_iota(jnp.int32, (slots // 128, 1), 0) == slot // 128
    low = lax.broadcasted_iota(jnp.int32, (128, 1), 0) == slot % 128
    meta = lax.dot_general(
        jnp.where(high, (tile + 1).astype(jnp.bfloat16), 0),
        low.astype(jnp.bfloat16),
        (((1,), (1,)), ((), ())),
        preferred_element_type=jnp.float32,
    )
    meta = meta.reshape(owners, capacity // 128, 128).astype(jnp.bfloat16)
    meta = jnp.pad(meta, ((0, 0), (0, META - capacity // 128), (0, 0)))
    return slot.reshape(count), meta


def on_device_fast(*args):
    return fast_step(*args)


def fast_step(preacts, targets, decoder, owner_list, tile_source, tile_target, row_order):
    owners = lax.axis_size("tile")
    my_half = lax.axis_index("feat")
    layers, feats, tokens = preacts.shape
    tiles = tile_source.shape[0]
    slots, width = decoder.shape[2:]
    capacity = slots // owners
    rows = layers * 8
    weights = decoder.reshape(slots, width)
    bf16, f32, i32 = jnp.bfloat16, jnp.float32, jnp.int32

    me = lax.axis_index("tile")
    slot, meta = slot_plan(owner_list ^ me, tiles, owners, capacity)
    me_id = jnp.reshape(me, (1,)).astype(i32)
    half_id = jnp.reshape(my_half, (1,)).astype(i32)
    block_of = lax.broadcasted_iota(i32, row_order.shape, 0) * row_order.shape[1]
    token_of = (row_order + block_of).reshape(tokens)
    perm = (token_of[:, None] == lax.broadcasted_iota(i32, (1, tokens), 1)).astype(bf16)
    index = lax.broadcasted_iota(i32, (1, layers * tokens), 1)
    side = jnp.where(index // (owners * rows) == 0, my_half, 1 - my_half)
    peer = lax.axis_index("tile") ^ (index % (owners * rows) // rows)
    held = peer * 16 + side * 8 + index % 8
    held_layer = index % rows // 8
    wanted = jnp.tile(token_of, layers)[:, None]
    wanted_layer = lax.broadcasted_iota(i32, (layers * tokens, 1), 0) // tokens
    place = ((held == wanted) & (held_layer == wanted_layer)).astype(bf16)
    tile_ids = jnp.arange(tiles, dtype=i32)
    earlier = (tile_source[None, :] < tile_source[:, None]) | (
        (tile_source[None, :] == tile_source[:, None]) & (tile_ids[None, :] < tile_ids[:, None])
    )
    position = jnp.sum(earlier.astype(i32), axis=1)
    order = jnp.sum(
        jnp.where(position[None, :] == tile_ids[:, None], tile_ids[None, :], 0), axis=1
    ).astype(i32)

    def to_peer(d, block):
        return lax.ppermute(block, "tile", [(q, q ^ d) for q in range(owners)])

    mirror = owners // 2
    near = range(1, mirror)
    block = jax.ShapeDtypeStruct((capacity + META, tokens), bf16)
    packed = pl.pallas_call(
        pack_kernel,
        out_shape=[block] * owners,
        grid_spec=pltpu.PrefetchScalarGridSpec(
            num_scalar_prefetch=2,
            grid=(1,),
            in_specs=[full(preacts.shape), full(perm.shape), full(meta.shape)],
            out_specs=[full(block.shape)] * owners,
            scratch_shapes=[
                pltpu.VMEM((layers * feats, tokens), f32),
                pltpu.VMEM((slots, tokens), f32),
            ],
        ),
        compiler_params=vmem(32),
    )(slot, tile_source, preacts, perm, meta)
    received = list(packed)
    for d in SEND_ORDER:
        received[d] = to_peer(d, packed[d])

    def cost(count):
        return pl.CostEstimate(
            flops=2 * layers * tokens * count * capacity * width,
            bytes_accessed=2 * count * capacity * width,
            transcendentals=0,
        )

    weight_spec = pl.BlockSpec(
        (capacity // SPLIT, width),
        lambda i, tgt, seq, me, *_: ((me[0] ^ seq[i // SPLIT]) * SPLIT + i % SPLIT, 0),
    )
    whole = pl.BlockSpec(memory_space=pltpu.VMEM)

    def forward(number, run, before, last):
        first, count = before is None, len(run)
        if last:
            outs = [
                jax.ShapeDtypeStruct((owners, rows - 8, width), f32),
                jax.ShapeDtypeStruct((owners, 8, width), f32),
            ] * 2
        else:
            outs = [jax.ShapeDtypeStruct((layers * tokens, width), f32)]
        sums = [] if first else [before]
        ready = [place, order] if number == 1 else []
        return pl.pallas_call(
            functools.partial(forward_kernel, count, first, last, len(ready)),
            out_shape=outs,
            grid_spec=pltpu.PrefetchScalarGridSpec(
                num_scalar_prefetch=4,
                grid=(count * SPLIT,),
                in_specs=[whole] * count
                + [weight_spec]
                + [whole] * len(sums)
                + [pl.BlockSpec(memory_space=pl.ANY)] * len(ready),
                out_specs=[full(o.shape) for o in outs] if last else [whole],
                scratch_shapes=[
                    pltpu.VMEM((layers * tokens, width), f32),
                    pltpu.VMEM((layers * tokens, capacity // SPLIT), bf16),
                    pltpu.VMEM((META, 128), f32),
                    pltpu.VMEM((capacity // SPLIT, tokens), bf16),
                ],
            ),
            compiler_params=vmem(28),
            cost_estimate=cost(count),
        )(
            tile_target,
            jnp.array(run, i32),
            me_id,
            half_id,
            *[received[d] for d in run],
            weights,
            *sums,
            *ready,
        )

    value = None
    for number, run in enumerate(FORWARD_RUNS):
        last = number == len(FORWARD_RUNS) - 1
        value = forward(number, run, value, last)
        if not last:
            value = value[0]

    swap = [(0, 1), (1, 0)]
    keep_most, keep_last, send_most, send_last = value
    got_last = lax.ppermute(send_last, "feat", swap)
    got_most = lax.ppermute(send_most, "feat", swap)
    last_sum = keep_last + got_last
    across = to_peer(mirror, last_sum[mirror:])
    most_sum = (keep_most + got_most).reshape(2, mirror, rows - 8, width)
    pair = most_sum[:, 0]
    for d in near:
        pair = pair + to_peer(d, most_sum[:, d])
    last_sum = last_sum[:mirror] + across
    own_last = last_sum[0]
    for d in near:
        own_last = own_last + to_peer(d, last_sum[d])
    own_most = pair[0] + to_peer(mirror, pair[1])
    wanted = targets.astype(f32).reshape(rows, width)
    own = [own_most - wanted[: rows - 8], own_last - wanted[rows - 8 :]]
    spread = jnp.concatenate([o.astype(bf16) for o in own])
    blocks = [spread] + [None] * (owners - 1)
    blocks[mirror] = to_peer(mirror, spread)
    for d in near:
        blocks[d] = to_peer(d, spread)
    for d in near:
        blocks[mirror + d] = to_peer(d, blocks[mirror])
    mine = jnp.concatenate(blocks)
    other = lax.ppermute(mine, "feat", swap)

    grad_block = jax.ShapeDtypeStruct((capacity, tokens), bf16)
    spread_type = jax.ShapeDtypeStruct((layers * tokens, width), bf16)
    meta_spec = pl.BlockSpec((META, tokens), lambda *_: (capacity // META, 0))

    def backward(run, known):
        first, count = len(known) > 1, len(run)
        outs = [grad_block] * count + ([spread_type] if first else [])
        return pl.pallas_call(
            functools.partial(backward_kernel, count, first),
            out_shape=outs,
            grid_spec=pltpu.PrefetchScalarGridSpec(
                num_scalar_prefetch=3,
                grid=(count * SPLIT,),
                in_specs=[meta_spec] * count + [weight_spec] + [whole] * len(known),
                out_specs=[whole] * len(outs),
                scratch_shapes=[
                    pltpu.VMEM((META, 128), f32),
                    pltpu.VMEM((capacity // SPLIT, tokens), bf16),
                ],
            ),
            compiler_params=vmem(28),
            cost_estimate=cost(count),
        )(
            tile_target,
            jnp.array(run, i32),
            me_id,
            *[received[d] for d in run],
            weights,
            *known,
        )

    returned = [None] * owners
    known = (mine, other, place)
    for run in BACKWARD_RUNS:
        grads = backward(run, known)
        if len(known) > 1:
            known = (grads[len(run)],)
        for d, grad in zip(run, grads):
            returned[d] = to_peer(d, grad) if d else grad

    feature_grad = pl.pallas_call(
        unpack_kernel,
        out_shape=jax.ShapeDtypeStruct(preacts.shape, f32),
        grid_spec=pltpu.PrefetchScalarGridSpec(
            num_scalar_prefetch=2,
            grid=(1,),
            in_specs=[pl.BlockSpec(memory_space=pltpu.HBM)] * owners + [full(preacts.shape)],
            out_specs=full(preacts.shape),
            scratch_shapes=[
                pltpu.VMEM((slots, tokens), f32),
                pltpu.VMEM((owners, capacity, tokens), bf16),
                pltpu.SemaphoreType.DMA((owners,)),
            ],
        ),
        compiler_params=vmem(60),
    )(slot, order, *returned, preacts)
    residual = jnp.concatenate(own).reshape(targets.shape)
    return residual, feature_grad


def on_device(preacts, targets, decoder, owner_list, tile_source, tile_target, row_order):
    args = (preacts, targets, decoder, owner_list, tile_source, tile_target, row_order)
    owners, halves = lax.axis_size("tile"), lax.axis_size("feat")
    layers, feat_dev, tokens = preacts.shape
    tile_count = tile_source.shape[0]
    slot_count, model_width = decoder.shape[2:]
    fits = (
        tokens == 128
        and halves == 2
        and tokens == 8 * owners * halves
        and slot_count % (owners * 256) == 0
        and slot_count <= owners * META * 128
        and (feat_dev * tile_count) % 128 == 0
        and feat_dev % UNROLL == 0
        and tile_count * 2 == layers * (layers + 1)
        and model_width % 256 == 0
    )
    return (on_device_fast if fits else on_device_general)(*args)


def solution(mesh):
    return jax.shard_map(
        on_device,
        mesh=mesh,
        in_specs=(
            P(None, ("tile", "feat"), "groups"),
            P(None, ("groups", "tile", "feat"), None),
            P(("groups", "tile"), "feat", None, None),
            P(("tile", "feat"), None, None),
            P(),
            P(),
            P("groups", None),
        ),
        out_specs=(P(None, ("groups", "tile", "feat"), None), P(None, ("tile", "feat"), "groups")),
        check_vma=False,
    )
```

```python
import functools

import jax
import jax.numpy as jnp
from jax import lax
from jax.experimental import pallas as pl
from jax.experimental.pallas import tpu as pltpu
from jax.sharding import PartitionSpec as P


META = 16
UNROLL = 16
NCOL = 768
SPLIT = 2
SEND_ORDER = (2, 1, 3, 4, 5, 6, 7)
FORWARD_RUNS = ((0,), (1, 2, 3), (4, 5), (6,), (7,))
BACKWARD_RUNS = ((4,), (5,), (6, 7), (3, 2, 1, 0))


def reorder(values, indices):
    leading = values.shape[:-1]
    blocks, block_span = indices.shape
    shaped = values.reshape(leading + (blocks, block_span))
    block_col = jnp.arange(blocks, dtype=jnp.int32)[:, None]
    return shaped[..., block_col, indices].reshape(values.shape)


def inverse_order(row_order):
    positions = lax.broadcasted_iota(jnp.int32, row_order.shape, 1)
    block_ids = lax.broadcasted_iota(jnp.int32, row_order.shape, 0)
    inverse = jnp.zeros(row_order.shape, jnp.int32)
    return inverse.at[block_ids, row_order].set(positions)


def on_device_general(preacts, targets, decoder, owner_list, tile_source, tile_target, row_order):
    owners = lax.axis_size("tile")
    layers, feat_dev, tokens = preacts.shape
    tile_count = tile_source.shape[0]
    slot_count = decoder.shape[2]
    capacity = slot_count // owners
    model_width = decoder.shape[3]
    inverse = inverse_order(row_order)
    active = jax.nn.relu(preacts.astype(jnp.float32)).astype(jnp.bfloat16)
    natural = reorder(active, inverse)
    picked = natural[tile_source]
    row_values = jnp.transpose(picked, (1, 0, 2)).reshape(feat_dev * tile_count, tokens)
    destination = owner_list.reshape(-1)
    count_rows = destination.shape[0]
    same_owner = destination[:, None] == destination[None, :]
    before = lax.broadcasted_iota(jnp.int32, (count_rows, count_rows), 0) < lax.broadcasted_iota(
        jnp.int32, (count_rows, count_rows), 1
    )
    slot_rank = jnp.sum((same_owner & before).astype(jnp.int32), axis=0)
    slot_of = destination * capacity + slot_rank
    slot_match = lax.broadcasted_iota(jnp.int32, (slot_count, count_rows), 0) == slot_of[None, :]
    packed = jnp.dot(
        slot_match.astype(jnp.bfloat16), row_values, preferred_element_type=jnp.float32
    ).astype(jnp.bfloat16)
    tile_of_row = lax.broadcasted_iota(jnp.int32, (feat_dev, tile_count), 1).reshape(-1)
    tile_slot = jnp.sum(jnp.where(slot_match, tile_of_row[None, :] + 1, 0), axis=1) - 1
    received, tile_recv = (
        lax.all_to_all(
            packed.reshape(owners, capacity, tokens),
            "tile",
            split_axis=0,
            concat_axis=0,
            tiled=True,
        ),
        lax.all_to_all(
            tile_slot.reshape(owners, capacity), "tile", split_axis=0, concat_axis=0, tiled=True
        ),
    )
    received = received.reshape(slot_count, tokens)
    tile_recv = tile_recv.reshape(slot_count)
    tile_ids = lax.broadcasted_iota(jnp.int32, (slot_count, tile_count), 1)
    target_slot = jnp.sum(
        jnp.where(tile_recv[:, None] == tile_ids, tile_target[None, :], 0), axis=1
    )
    occupied = tile_recv >= 0
    weights = decoder[0, 0]
    pieces = []
    for target_layer in range(layers):
        chosen = (occupied & (target_slot == target_layer))[:, None]
        masked = jnp.where(chosen, received, jnp.zeros_like(received))
        pieces.append(
            lax.dot_general(
                masked, weights, (((0,), (0,)), ((), ())), preferred_element_type=jnp.float32
            )
        )
    partial_value = jnp.stack(pieces).reshape(layers, 2 * tokens, model_width // 2)
    own_sums = lax.psum_scatter(partial_value, ("tile", "feat"), scatter_dimension=1, tiled=True)
    residual = own_sums - targets.astype(jnp.float32)
    spread = lax.all_gather(
        residual.astype(jnp.bfloat16), ("tile", "feat"), axis=1, tiled=True
    ).reshape(layers, tokens, model_width)
    slot_grad = jnp.zeros((slot_count, tokens), jnp.float32)
    for target_layer in range(layers):
        chosen = (occupied & (target_slot == target_layer))[:, None]
        product = lax.dot_general(
            weights,
            spread[target_layer],
            (((1,), (1,)), ((), ())),
            preferred_element_type=jnp.float32,
        )
        slot_grad = slot_grad + jnp.where(chosen, product, 0.0)
    returned = lax.all_to_all(
        slot_grad.reshape(owners, capacity, tokens), "tile", split_axis=0, concat_axis=0, tiled=True
    ).reshape(slot_count, tokens)
    row_grad = returned[slot_of].reshape(feat_dev, tile_count, tokens)
    layer_grad = jnp.stack(
        [
            jnp.sum(jnp.where((tile_source == source_layer)[None, :, None], row_grad, 0.0), axis=1)
            for source_layer in range(layers)
        ]
    )
    natural_pre = reorder(preacts, inverse)
    layer_grad = jnp.where(natural_pre > 0, layer_grad, 0.0)
    feature_grad = reorder(layer_grad, row_order)
    return (residual, feature_grad)


def vmem(limit=60):
    return pltpu.CompilerParams(vmem_limit_bytes=limit * 2**20)


def full(shape):
    return pl.BlockSpec(shape, lambda *_: (0,) * len(shape))


def pack_kernel(slot_sm, src_sm, pre_ref, perm_ref, meta_ref, *refs):
    outs, (nat, packed) = refs[:-2], refs[-2:]
    layers, feats, _ = pre_ref.shape
    tiles = src_sm.shape[0]
    capacity = packed.shape[0] // len(outs)
    for s in range(layers):
        active = jnp.maximum(pre_ref[s].astype(jnp.float32), 0.0).astype(jnp.bfloat16)
        nat[pl.ds(s * feats, feats), :] = jnp.dot(
            active, perm_ref[...], preferred_element_type=jnp.float32
        )
    bases = [src_sm[k] * feats for k in range(tiles)]

    def step(i, carry):
        unit = i * (UNROLL * tiles)
        at = [base + i * UNROLL for base in bases]
        for j in range(UNROLL):
            for k in range(tiles):
                slot = slot_sm[unit + (j * tiles + k)]
                packed[pl.ds(slot, 1), :] = nat[pl.ds(at[k] + j, 1), :]
        return carry

    lax.fori_loop(0, feats // UNROLL, step, 0)
    for d, out_ref in enumerate(outs):
        out_ref[:capacity, :] = packed[d * capacity : (d + 1) * capacity, :].astype(jnp.bfloat16)
        out_ref[capacity:, :] = meta_ref[d]


def slot_targets(meta, tgt_sm):
    values = meta.astype(jnp.float32)
    target = jnp.full(values.shape, -1.0, jnp.float32)
    for k in range(tgt_sm.shape[0]):
        target = jnp.where(values == float(k + 1), tgt_sm[k].astype(jnp.float32), target)
    return target


def forward_kernel(count, first, last, ready, tgt_sm, seq_sm, me_sm, half_sm, *refs):
    recv_refs, w_ref, refs = refs[:count], refs[count], refs[count + 1 :]
    if not first:
        before_ref, refs = refs[0], refs[1 + ready :]
    outs, (acc, lhs, goal, stage) = refs[:-4], refs[-4:]
    i = pl.program_id(0)
    depth, width = w_ref.shape
    capacity = depth * SPLIT
    tokens = recv_refs[0].shape[1]
    layers = lhs.shape[0] // tokens
    groups = depth // 128
    for n in range(count * SPLIT):

        @pl.when(i == n)
        def _():
            recv_ref, first_row = recv_refs[n // SPLIT], n % SPLIT * groups
            target = slot_targets(recv_ref[capacity:, :], tgt_sm)
            goal[:groups, :] = target[first_row : first_row + groups, :]
            stage[...] = recv_ref[first_row * 128 : (first_row + groups) * 128, :]

    for j in range(groups):
        span = slice(j * 128, (j + 1) * 128)
        acts = stage[span, :].astype(jnp.float32).T
        for t in range(layers):
            lhs[t * tokens : (t + 1) * tokens, span] = jnp.where(
                goal[j : j + 1, :] == float(t), acts, 0.0
            ).astype(jnp.bfloat16)

    @pl.when(i == 0)
    def _():
        acc[...] = jnp.zeros_like(acc) if first else before_ref[...]

    for n in range(width // NCOL):
        cols = slice(n * NCOL, (n + 1) * NCOL)
        acc[:, cols] += jnp.dot(lhs[...], w_ref[:, cols], preferred_element_type=jnp.float32)

    @pl.when(i == count * SPLIT - 1)
    def _():
        if not last:
            outs[0][...] = acc[...]
            return
        owners = outs[0].shape[0]
        for d in range(owners):
            for t in range(layers):
                for side, half in enumerate((half_sm[0], 1 - half_sm[0])):
                    place = pl.multiple_of(t * tokens + (me_sm[0] ^ d) * 16 + half * 8, 8)
                    values = acc[pl.ds(place, 8), :]
                    if t < layers - 1:
                        outs[2 * side][d, t * 8 : (t + 1) * 8, :] = values
                    else:
                        outs[2 * side + 1][d] = values


def backward_kernel(count, first, tgt_sm, seq_sm, me_sm, *all_refs):
    refs = all_refs
    meta_refs, w_ref, refs = refs[:count], refs[count], refs[count + 1 : -2]
    goal, stage = all_refs[-2:]
    i = pl.program_id(0)
    if first:
        mine_ref, other_ref, place_ref = refs[:3]
        outs, spread = refs[3:-1], refs[-1]
        half = mine_ref.shape[0]

        @pl.when(i == 0)
        def _():
            spread[...] = (
                jnp.dot(place_ref[:, :half], mine_ref[...], preferred_element_type=jnp.float32)
                + jnp.dot(place_ref[:, half:], other_ref[...], preferred_element_type=jnp.float32)
            ).astype(jnp.bfloat16)

    else:
        spread, outs = refs[0], refs[1:]
    depth = w_ref.shape[0]
    tokens = outs[0].shape[1]
    layers = spread.shape[0] // tokens
    groups = depth // 128
    for n in range(count * SPLIT):

        @pl.when(i == n)
        def _():
            first_row = n % SPLIT * groups
            target = slot_targets(meta_refs[n // SPLIT][...], tgt_sm)
            goal[:groups, :] = target[first_row : first_row + groups, :]

    for j in range(depth // 256):
        grads = lax.dot_general(
            spread[...],
            w_ref[j * 256 : (j + 1) * 256, :],
            (((1,), (1,)), ((), ())),
            preferred_element_type=jnp.float32,
        )
        for h in range(2):
            row = goal[2 * j + h : 2 * j + h + 1, :]
            chosen = jnp.zeros((tokens, 128), jnp.float32)
            for t in range(layers):
                part = grads[t * tokens : (t + 1) * tokens, h * 128 : (h + 1) * 128]
                chosen = jnp.where(row == float(t), part, chosen)
            begin = j * 256 + h * 128
            stage[begin : begin + 128, :] = chosen.T.astype(jnp.bfloat16)
    for n in range(count * SPLIT):

        @pl.when(i == n)
        def _():
            outs[n // SPLIT][n % SPLIT * depth : (n % SPLIT + 1) * depth, :] = stage[...]


def unpack_kernel(slot_sm, order_sm, *refs):
    backs, (pre_ref, out_ref, rows, landed, sems) = refs[:-5], refs[-5:]
    layers, feats, _ = pre_ref.shape
    tiles = order_sm.shape[0]
    capacity = rows.shape[0] // len(backs)
    copies = [
        pltpu.make_async_copy(back_ref, landed.at[d], sems.at[d])
        for d, back_ref in enumerate(backs)
    ]
    for copy in copies:
        copy.start()
    for d, copy in enumerate(copies):
        copy.wait()
        rows[d * capacity : (d + 1) * capacity, :] = landed[d].astype(jnp.float32)
    order = [order_sm[k] for k in range(tiles)]

    def step(i, carry):
        at = [i * (UNROLL * tiles) + o for o in order]
        for j in range(UNROLL):
            f = i * UNROLL + j
            k = 0
            for s in range(layers):
                total = None
                for _ in range(layers - s):
                    row = rows[pl.ds(slot_sm[at[k] + j * tiles], 1), :]
                    total = row if total is None else total + row
                    k += 1
                out_ref[s, pl.ds(f, 1), :] = total
        return carry

    lax.fori_loop(0, feats // UNROLL, step, 0)
    for s in range(layers):
        out_ref[s] = jnp.where(pre_ref[s].astype(jnp.float32) > 0, out_ref[s], 0.0)


def slot_plan(owner_list, tile_count, owners, capacity):
    count = owner_list.size
    blocks = count // 128
    dest = owner_list.reshape(blocks, 128)
    same = dest[None] == lax.broadcasted_iota(jnp.int32, (owners, 1, 1), 0)
    ones = same.astype(jnp.bfloat16)
    lane = lax.broadcasted_iota(jnp.int32, (128, 128), 0) < lax.broadcasted_iota(
        jnp.int32, (128, 128), 1
    )
    ahead = lax.broadcasted_iota(jnp.int32, (blocks, blocks), 0) < lax.broadcasted_iota(
        jnp.int32, (blocks, blocks), 1
    )
    within = jnp.einsum(
        "pbi,ij->pbj", ones, lane.astype(jnp.bfloat16), preferred_element_type=jnp.float32
    )
    totals = jnp.sum(ones, axis=2, dtype=jnp.float32).astype(jnp.bfloat16)
    base = jnp.dot(totals, ahead.astype(jnp.bfloat16), preferred_element_type=jnp.float32)
    rank = jnp.sum(jnp.where(same, within + base[:, :, None], 0.0), axis=0).astype(jnp.int32)
    slot = (dest * capacity + rank).reshape(1, count)
    slots = owners * capacity
    tile = lax.broadcasted_iota(jnp.int32, (1, count), 1) % tile_count
    high = lax.broadcasted_iota(jnp.int32, (slots // 128, 1), 0) == slot // 128
    low = lax.broadcasted_iota(jnp.int32, (128, 1), 0) == slot % 128
    meta = lax.dot_general(
        jnp.where(high, (tile + 1).astype(jnp.bfloat16), 0),
        low.astype(jnp.bfloat16),
        (((1,), (1,)), ((), ())),
        preferred_element_type=jnp.float32,
    )
    meta = meta.reshape(owners, capacity // 128, 128).astype(jnp.bfloat16)
    meta = jnp.pad(meta, ((0, 0), (0, META - capacity // 128), (0, 0)))
    return slot.reshape(count), meta


def on_device_fast(*args):
    return fast_step(*args)


def fast_step(preacts, targets, decoder, owner_list, tile_source, tile_target, row_order):
    owners = lax.axis_size("tile")
    my_half = lax.axis_index("feat")
    layers, feats, tokens = preacts.shape
    tiles = tile_source.shape[0]
    slots, width = decoder.shape[2:]
    capacity = slots // owners
    rows = layers * 8
    weights = decoder.reshape(slots, width)
    bf16, f32, i32 = jnp.bfloat16, jnp.float32, jnp.int32

    me = lax.axis_index("tile")
    slot, meta = slot_plan(owner_list ^ me, tiles, owners, capacity)
    me_id = jnp.reshape(me, (1,)).astype(i32)
    half_id = jnp.reshape(my_half, (1,)).astype(i32)
    block_of = lax.broadcasted_iota(i32, row_order.shape, 0) * row_order.shape[1]
    token_of = (row_order + block_of).reshape(tokens)
    perm = (token_of[:, None] == lax.broadcasted_iota(i32, (1, tokens), 1)).astype(bf16)
    index = lax.broadcasted_iota(i32, (1, layers * tokens), 1)
    side = jnp.where(index // (owners * rows) == 0, my_half, 1 - my_half)
    peer = lax.axis_index("tile") ^ (index % (owners * rows) // rows)
    held = peer * 16 + side * 8 + index % 8
    held_layer = index % rows // 8
    wanted = jnp.tile(token_of, layers)[:, None]
    wanted_layer = lax.broadcasted_iota(i32, (layers * tokens, 1), 0) // tokens
    place = ((held == wanted) & (held_layer == wanted_layer)).astype(bf16)
    tile_ids = jnp.arange(tiles, dtype=i32)
    earlier = (tile_source[None, :] < tile_source[:, None]) | (
        (tile_source[None, :] == tile_source[:, None]) & (tile_ids[None, :] < tile_ids[:, None])
    )
    position = jnp.sum(earlier.astype(i32), axis=1)
    order = jnp.sum(
        jnp.where(position[None, :] == tile_ids[:, None], tile_ids[None, :], 0), axis=1
    ).astype(i32)

    def to_peer(d, block):
        return lax.ppermute(block, "tile", [(q, q ^ d) for q in range(owners)])

    mirror = owners // 2
    near = range(1, mirror)
    block = jax.ShapeDtypeStruct((capacity + META, tokens), bf16)
    packed = pl.pallas_call(
        pack_kernel,
        out_shape=[block] * owners,
        grid_spec=pltpu.PrefetchScalarGridSpec(
            num_scalar_prefetch=2,
            grid=(1,),
            in_specs=[full(preacts.shape), full(perm.shape), full(meta.shape)],
            out_specs=[full(block.shape)] * owners,
            scratch_shapes=[
                pltpu.VMEM((layers * feats, tokens), f32),
                pltpu.VMEM((slots, tokens), f32),
            ],
        ),
        compiler_params=vmem(32),
    )(slot, tile_source, preacts, perm, meta)
    received = list(packed)
    for d in SEND_ORDER:
        received[d] = to_peer(d, packed[d])

    def cost(count):
        return pl.CostEstimate(
            flops=2 * layers * tokens * count * capacity * width,
            bytes_accessed=2 * count * capacity * width,
            transcendentals=0,
        )

    weight_spec = pl.BlockSpec(
        (capacity // SPLIT, width),
        lambda i, tgt, seq, me, *_: ((me[0] ^ seq[i // SPLIT]) * SPLIT + i % SPLIT, 0),
    )
    whole = pl.BlockSpec(memory_space=pltpu.VMEM)

    def forward(number, run, before, last):
        first, count = before is None, len(run)
        if last:
            outs = [
                jax.ShapeDtypeStruct((owners, rows - 8, width), f32),
                jax.ShapeDtypeStruct((owners, 8, width), f32),
            ] * 2
        else:
            outs = [jax.ShapeDtypeStruct((layers * tokens, width), f32)]
        sums = [] if first else [before]
        ready = [place, order] if number == 1 else []
        return pl.pallas_call(
            functools.partial(forward_kernel, count, first, last, len(ready)),
            out_shape=outs,
            grid_spec=pltpu.PrefetchScalarGridSpec(
                num_scalar_prefetch=4,
                grid=(count * SPLIT,),
                in_specs=[whole] * count
                + [weight_spec]
                + [whole] * len(sums)
                + [pl.BlockSpec(memory_space=pl.ANY)] * len(ready),
                out_specs=[full(o.shape) for o in outs] if last else [whole],
                scratch_shapes=[
                    pltpu.VMEM((layers * tokens, width), f32),
                    pltpu.VMEM((layers * tokens, capacity // SPLIT), bf16),
                    pltpu.VMEM((META, 128), f32),
                    pltpu.VMEM((capacity // SPLIT, tokens), bf16),
                ],
            ),
            compiler_params=vmem(28),
            cost_estimate=cost(count),
        )(
            tile_target,
            jnp.array(run, i32),
            me_id,
            half_id,
            *[received[d] for d in run],
            weights,
            *sums,
            *ready,
        )

    value = None
    for number, run in enumerate(FORWARD_RUNS):
        last = number == len(FORWARD_RUNS) - 1
        value = forward(number, run, value, last)
        if not last:
            value = value[0]

    swap = [(0, 1), (1, 0)]
    keep_most, keep_last, send_most, send_last = value
    got_last = lax.ppermute(send_last, "feat", swap)
    got_most = lax.ppermute(send_most, "feat", swap)
    last_sum = keep_last + got_last
    across = to_peer(mirror, last_sum[mirror:])
    most_sum = (keep_most + got_most).reshape(2, mirror, rows - 8, width)
    pair = most_sum[:, 0]
    for d in near:
        pair = pair + to_peer(d, most_sum[:, d])
    last_sum = last_sum[:mirror] + across
    own_last = last_sum[0]
    for d in near:
        own_last = own_last + to_peer(d, last_sum[d])
    own_most = pair[0] + to_peer(mirror, pair[1])
    wanted = targets.astype(f32).reshape(rows, width)
    own = [own_most - wanted[: rows - 8], own_last - wanted[rows - 8 :]]
    spread = jnp.concatenate([o.astype(bf16) for o in own])
    blocks = [spread] + [None] * (owners - 1)
    blocks[mirror] = to_peer(mirror, spread)
    for d in near:
        blocks[d] = to_peer(d, spread)
    for d in near:
        blocks[mirror + d] = to_peer(d, blocks[mirror])
    mine = jnp.concatenate(blocks)
    other = lax.ppermute(mine, "feat", swap)

    grad_block = jax.ShapeDtypeStruct((capacity, tokens), bf16)
    spread_type = jax.ShapeDtypeStruct((layers * tokens, width), bf16)
    meta_spec = pl.BlockSpec((META, tokens), lambda *_: (capacity // META, 0))

    def backward(run, known):
        first, count = len(known) > 1, len(run)
        outs = [grad_block] * count + ([spread_type] if first else [])
        return pl.pallas_call(
            functools.partial(backward_kernel, count, first),
            out_shape=outs,
            grid_spec=pltpu.PrefetchScalarGridSpec(
                num_scalar_prefetch=3,
                grid=(count * SPLIT,),
                in_specs=[meta_spec] * count + [weight_spec] + [whole] * len(known),
                out_specs=[whole] * len(outs),
                scratch_shapes=[
                    pltpu.VMEM((META, 128), f32),
                    pltpu.VMEM((capacity // SPLIT, tokens), bf16),
                ],
            ),
            compiler_params=vmem(28),
            cost_estimate=cost(count),
        )(
            tile_target,
            jnp.array(run, i32),
            me_id,
            *[received[d] for d in run],
            weights,
            *known,
        )

    returned = [None] * owners
    known = (mine, other, place)
    for run in BACKWARD_RUNS:
        grads = backward(run, known)
        if len(known) > 1:
            known = (grads[len(run)],)
        for d, grad in zip(run, grads):
            returned[d] = to_peer(d, grad) if d else grad

    feature_grad = pl.pallas_call(
        unpack_kernel,
        out_shape=jax.ShapeDtypeStruct(preacts.shape, f32),
        grid_spec=pltpu.PrefetchScalarGridSpec(
            num_scalar_prefetch=2,
            grid=(1,),
            in_specs=[pl.BlockSpec(memory_space=pltpu.HBM)] * owners + [full(preacts.shape)],
            out_specs=full(preacts.shape),
            scratch_shapes=[
                pltpu.VMEM((slots, tokens), f32),
                pltpu.VMEM((owners, capacity, tokens), bf16),
                pltpu.SemaphoreType.DMA((owners,)),
            ],
        ),
        compiler_params=vmem(60),
    )(slot, order, *returned, preacts)
    residual = jnp.concatenate(own).reshape(targets.shape)
    return residual, feature_grad


def on_device(preacts, targets, decoder, owner_list, tile_source, tile_target, row_order):
    args = (preacts, targets, decoder, owner_list, tile_source, tile_target, row_order)
    owners, halves = lax.axis_size("tile"), lax.axis_size("feat")
    layers, feat_dev, tokens = preacts.shape
    tile_count = tile_source.shape[0]
    slot_count, model_width = decoder.shape[2:]
    fits = (
        tokens == 128
        and halves == 2
        and tokens == 8 * owners * halves
        and slot_count % (owners * 256) == 0
        and slot_count <= owners * META * 128
        and (feat_dev * tile_count) % 128 == 0
        and feat_dev % UNROLL == 0
        and tile_count * 2 == layers * (layers + 1)
        and model_width % 256 == 0
    )
    return (on_device_fast if fits else on_device_general)(*args)


def solution(mesh):
    return jax.shard_map(
        on_device,
        mesh=mesh,
        in_specs=(
            P(None, ("tile", "feat"), "groups"),
            P(None, ("groups", "tile", "feat"), None),
            P(("groups", "tile"), "feat", None, None),
            P(("tile", "feat"), None, None),
            P(),
            P(),
            P("groups", None),
        ),
        out_specs=(P(None, ("groups", "tile", "feat"), None), P(None, ("tile", "feat"), "groups")),
        check_vma=False,
    )
```
